32 devices in a mesh: group: 8 (over y, x, core), tile: 4 (over z).
Axes of the slice: x: 2, y: 2, z: 4, core: 2. Of those that a mesh axis runs over, the one named last changes fastest.
Arguments:
- coupling: float32 [32, 1024, 768], P('group', None, 'tile'), may hold values from -6 to 6
- interior_solve: float32 [32, 768, 1024], P('group', 'tile'), may hold values from -0.21875 to 0.21875
- boundary_stiffness: float32 [32, 1024, 1024], P('group', 'tile'), may hold values from -6 to 6
- migration: int32 [32], replicated, may hold values from -1 to 15, as said below
Outputs:
- condensed: float32 [16, 1024, 1024], P('group', 'tile')
The draws below stay inside these ranges and needn't reach their ends.
Inputs may be any that keep to these rules, and one draw needn't show every extreme that they name: `migration`: every condensed slot is named by exactly one RVE slot; RVE slots of group g are g * 4 to g * 4 + 3; the condensed slots of group g are named only by RVE slots of group g or of its partner, the group whose index differs from g in the lowest bit; some group holds 4 plastic RVEs.
All inputs are finite; a program needn't handle non-finite values.
Results may differ from the reference program's by a relative error of at most 0.000071.
Values sent between devices are 32-bit elements; how exact they have to be, the bound alone decides.
A program may use at most 64 MiB of HBM per device.

```python
import jax
import jax.numpy as jnp
from jax import lax

BOUNDARY = 1024
INTERIOR = 768
OWN = 2
HOME = 4
RVES = 32
SLOTS = 16


def draw_migration(key, part):
    groups = RVES // HOME
    couples = groups // 2
    key_heavy, key_slots = jax.random.split(jax.random.fold_in(key, 23))
    heavy_bit = jax.random.randint(key_heavy, (couples,), 0, 2).astype(jnp.int32)
    couple_ids = jnp.arange(couples, dtype=jnp.int32)
    heavies = 2 * couple_ids + heavy_bit
    lights = 2 * couple_ids + 1 - heavy_bit
    slot_ids = jnp.arange(OWN, dtype=jnp.int32)[None, :]
    targets = jnp.concatenate([heavies[:, None] * OWN + slot_ids, lights[:, None] * OWN + slot_ids], axis=1)
    subkeys = jax.random.split(key_slots, couples)
    shuffles = jax.vmap(lambda sub_key: jax.random.permutation(sub_key, HOME))(subkeys).astype(jnp.int32)
    places = heavies[:, None] * HOME + shuffles
    result = jnp.full((RVES,), -1, jnp.int32)
    return result.at[places.reshape(-1)].set(targets.reshape(-1).astype(jnp.int32))


def block_scale(key, extent, shards, least, largest):
    level = 1.0
    for dim, parts in shards:
        steps = jax.random.uniform(jax.random.fold_in(jax.random.fold_in(key, 6), dim), (parts,), jnp.float32, least / len(shards), largest / len(shards))
        level = level * jnp.repeat(jnp.exp(steps), extent[dim] // parts).reshape((-1,) + (1,) * (len(extent) - 1 - dim))
    return level


def scatter_about(rng, dims, spread, bound, cuts=(), kind=jnp.bfloat16):
    drawn = spread * jax.random.normal(rng, dims, jnp.float32)
    if cuts:
        drawn = drawn * block_scale(rng, dims, cuts, -0.22, 0.18)
    return jnp.clip(drawn, -bound, bound).astype(kind)


def setup_inputs(seed: int = 0) -> dict:
    arg_keys = jax.random.split(jax.random.key(seed), 5)
    return {
        "coupling": scatter_about(arg_keys[0], (RVES, BOUNDARY, INTERIOR), 1.0, 6.0, ((0, 8), (2, 4)), jnp.float32),
        "interior_solve": scatter_about(arg_keys[1], (RVES, INTERIOR, BOUNDARY), INTERIOR ** -0.5, 0.21875, ((0, 8), (1, 4)), jnp.float32),
        "boundary_stiffness": scatter_about(arg_keys[2], (RVES, BOUNDARY, BOUNDARY), 1.0, 6.0, ((0, 8), (1, 4)), jnp.float32),
        "migration": draw_migration(jax.random.fold_in(arg_keys[4], 71), 0),
    }


def reference(coupling, interior_solve, boundary_stiffness, migration):
    targets = jnp.where(migration >= 0, migration, SLOTS).astype(jnp.int32)
    sources = jnp.zeros((SLOTS,), jnp.int32).at[targets].set(jnp.arange(RVES, dtype=jnp.int32), mode="drop")

    def condense_one(source):
        product = jnp.dot(coupling[source], interior_solve[source], precision=lax.Precision.HIGHEST, preferred_element_type=jnp.float32)
        return boundary_stiffness[source] - product

    return lax.map(condense_one, sources)
```

```python
import jax
import jax.numpy as jnp
from jax import lax
from jax.experimental import pallas as pl
from jax.experimental.pallas import tpu as pltpu
from jax.sharding import PartitionSpec as P

OWN = 2


def swapped(array, axis, distance):
    return lax.ppermute(array, axis, [(i, i ^ 1 << distance) for i in range(lax.axis_size(axis))])


def condense(coupling_cols, solve_rows, stiff_rows):
    product = lax.psum_scatter(
        jnp.dot(
            coupling_cols,
            solve_rows,
            precision=lax.Precision.HIGHEST,
            preferred_element_type=jnp.float32,
        ),
        "tile",
        scatter_dimension=0,
        tiled=True,
    )
    return stiff_rows - product


def select_slots(stacked, positions, present):
    chosen = jnp.take(stacked, positions, axis=0)
    shaped = present.reshape((-1,) + (1,) * (stacked.ndim - 1))
    return jnp.where(shaped, chosen, jnp.zeros_like(chosen))


def portable_body(coupling, interior_solve, boundary_stiffness, migration):
    home_count = coupling.shape[0]
    mygroup = lax.axis_index("group")
    partner = jnp.bitwise_xor(mygroup, 1)
    own_plan = lax.dynamic_slice_in_dim(migration, mygroup * home_count, home_count)
    slot_ids = jnp.arange(OWN, dtype=jnp.int32)
    local_ids = jnp.arange(home_count, dtype=jnp.int32)

    def locate(wanted):
        matches = own_plan[None, :] == wanted[:, None]
        positions = jnp.sum(jnp.where(matches, local_ids[None, :], 0), axis=1)
        return (positions, jnp.any(matches, axis=1))

    mine_index, mine_here = locate(mygroup * OWN + slot_ids)
    their_index, their_here = locate(partner * OWN + slot_ids)
    keep_mask = mine_here[:, None, None]
    outgoing = (
        select_slots(coupling, their_index, their_here),
        select_slots(interior_solve, their_index, their_here),
        select_slots(boundary_stiffness, their_index, their_here),
    )
    arrived = swapped((outgoing[0], outgoing[1], outgoing[2]), "group", 0)
    kept_coupling = jnp.where(keep_mask, jnp.take(coupling, mine_index, axis=0), arrived[0])
    kept_solve = jnp.where(keep_mask, jnp.take(interior_solve, mine_index, axis=0), arrived[1])
    kept_stiff = jnp.where(keep_mask, jnp.take(boundary_stiffness, mine_index, axis=0), arrived[2])
    result = jnp.stack(
        [condense(kept_coupling[slot], kept_solve[slot], kept_stiff[slot]) for slot in range(OWN)]
    )
    return result


MESH = pl.DeviceIdType.MESH
LINE = 4
CHUNKS = 4
STRIP = 16


def split_into(stack, slot, base, depth, rows, cols, value, order):
    high = value.astype(jnp.bfloat16)
    low = (value - high.astype(jnp.float32)).astype(jnp.bfloat16)
    for place, term in enumerate(order):
        at = pl.ds(base + place * depth + rows, value.shape[0])
        stack[slot, at, cols] = high if term == 0 else low


def contract(left, right):
    return lax.dot_general(left, right, (((0,), (0,)), ((), ())), preferred_element_type=jnp.float32)


def line_kernel(
    plan, k_hbm, x_hbm, b_hbm, out_hbm,
    k_home, x_home, b_home, k_out, x_out, b_out, k_in, x_in, b_in, k_got, x_got,
    k_end, x_end, k_stack, x_stack, p_send, p_recv, e_send, e_recv, result,
    load_sem, mig_send, mig_recv, em_send, em_recv, mm_send, mm_recv, me_send, me_recv, out_sem,
):
    home, depth, columns = x_home.shape
    rows = b_home.shape[1]
    width = columns // CHUNKS
    last = LINE - 1
    g, t = lax.axis_index("group"), lax.axis_index("tile")
    partner = g + 1 - 2 * (g % 2)
    middle = (t % last + last - 1) // last
    is_end = middle == 0
    is_mid = middle == 1
    mid = 1 + t // last
    end = (t - 1) * last
    across = last - t
    far_end_of_end = last - t
    far_mid_of_end = last - mid
    far_end_of_mid = (2 - t) * last

    def block(index):
        return pl.ds(pl.multiple_of(index * rows, rows), rows)

    def chunk(index):
        return pl.ds(pl.multiple_of(index * width, width), width)

    loads = [
        pltpu.make_async_copy(src, dst, load_sem.at[i])
        for i, (src, dst) in enumerate(((k_hbm, k_home), (x_hbm, x_home), (b_hbm, b_home)))
    ]
    for load in loads:
        load.start()

    barrier = pltpu.get_barrier_semaphore()
    pl.semaphore_signal(barrier, inc=1, device_id=(partner, t), device_id_type=MESH)

    @pl.when(is_end)
    def _():
        pl.semaphore_signal(barrier, inc=1, device_id=(g, mid), device_id_type=MESH)

    @pl.when(is_mid)
    def _():
        pl.semaphore_signal(barrier, inc=1, device_id=(g, end), device_id_type=MESH)
        pl.semaphore_signal(barrier, inc=1, device_id=(g, across), device_id_type=MESH)

    def find(wanted):
        index, here = jnp.int32(0), jnp.int32(0)
        for j in range(home):
            hit = plan[g * home + j] == wanted
            index, here = jnp.where(hit, j, index), jnp.where(hit, 1, here)
        return index, here > 0

    mine = [find(g * OWN + s) for s in range(OWN)]
    theirs = [find(partner * OWN + s) for s in range(OWN)]

    def migrate(s, kind):
        src, dst = ((k_out, k_in), (x_out, x_in), (b_out, b_in))[kind]
        return pltpu.make_async_remote_copy(
            src_ref=src.at[s], dst_ref=dst.at[s], send_sem=mig_send.at[s, kind], recv_sem=mig_recv.at[s, kind],
            device_id=(partner, t), device_id_type=MESH,
        )

    def gather(src, dst, count):
        for s in range(OWN):
            @pl.loop(0, count // STRIP)
            def _(i):
                at = pl.ds(pl.multiple_of(i * STRIP, STRIP), STRIP)
                dst[s, at, :] = src[theirs[s][0], at, :]

    loads[0].wait()
    gather(k_home, k_out, depth)
    loads[1].wait()
    gather(x_home, x_out, depth)

    @pl.when(is_end)
    def _():
        pl.semaphore_wait(barrier, 2)

    @pl.when(is_mid)
    def _():
        pl.semaphore_wait(barrier, 3)

    for s in range(OWN):
        for kind in range(2):
            migrate(s, kind).start()

    def settle(s):
        migrate(s, 0).wait_recv()
        migrate(s, 1).wait_recv()
        index, here = mine[s]

        @pl.loop(0, depth // STRIP)
        def _(i):
            at = pl.ds(pl.multiple_of(i * STRIP, STRIP), STRIP)
            k_got[s, at, :] = jnp.where(here, k_home[index, at, :], k_in[s, at, :])
            x_got[s, at, :] = jnp.where(here, x_home[index, at, :], x_in[s, at, :])

    def stack_own(s):
        @pl.loop(0, depth // STRIP)
        def _(i):
            first = pl.multiple_of(i * STRIP, STRIP)
            at = pl.ds(first, STRIP)
            everything = slice(None)
            split_into(k_stack, s, 0, depth, first, everything, k_got[s, at, :], (0, 0, 1))
            split_into(x_stack, s, 0, depth, first, everything, x_got[s, at, :], (0, 1, 0))

    def send_stiffness():
        loads[2].wait()
        gather(b_home, b_out, rows)
        for s in range(OWN):
            migrate(s, 2).start()

    def stiffness(s, c):
        index, here = mine[s]
        return jnp.where(here, b_home[index, :, chunk(c)], b_in[s, :, chunk(c)])

    def feed_k(s, j):
        target = (far_end_of_end, far_mid_of_end, mid)[j]
        return pltpu.make_async_remote_copy(
            src_ref=k_got.at[s, :, block(target)], dst_ref=k_end.at[s, j],
            send_sem=em_send.at[s, j], recv_sem=em_recv.at[s, j], device_id=(g, mid), device_id_type=MESH,
        )

    def feed_x(s, c):
        return pltpu.make_async_remote_copy(
            src_ref=x_got.at[s, :, chunk(c)], dst_ref=x_end.at[s, :, chunk(c)],
            send_sem=em_send.at[s, last + c], recv_sem=em_recv.at[s, last + c],
            device_id=(g, mid), device_id_type=MESH,
        )

    def cross(s, j, c):
        return pltpu.make_async_remote_copy(
            src_ref=p_send.at[s, j, c], dst_ref=p_recv.at[s, j, c],
            send_sem=mm_send.at[s, j, c], recv_sem=mm_recv.at[s, j, c],
            device_id=(g, across), device_id_type=MESH,
        )

    def deliver(s, c):
        return pltpu.make_async_remote_copy(
            src_ref=e_send.at[s, c], dst_ref=e_recv.at[s, c],
            send_sem=me_send.at[s, c], recv_sem=me_recv.at[s, c],
            device_id=(g, end), device_id_type=MESH,
        )

    def write(s, c):
        return pltpu.make_async_copy(
            result.at[s, :, chunk(c)], out_hbm.at[s, :, chunk(c)], out_sem.at[s, c]
        )

    own_terms = pl.ds(0, 3 * depth)

    @pl.when(is_end)
    def _():
        for s in range(OWN):
            settle(s)
            feed_k(s, 0).start()
            for c in range(CHUNKS):
                feed_x(s, c).start()
            feed_k(s, 1).start()
            feed_k(s, 2).start()
        send_stiffness()
        for s in range(OWN):
            stack_own(s)
        for s in range(OWN):
            migrate(s, 2).wait_recv()

            @pl.loop(0, CHUNKS)
            def _(c):
                result[s, :, chunk(c)] = stiffness(s, c) - contract(
                    k_stack[s, own_terms, block(t)], x_stack[s, own_terms, chunk(c)]
                )

        for s in range(OWN):
            @pl.loop(0, CHUNKS)
            def _(c):
                pltpu.make_async_remote_copy(
                    src_ref=e_send.at[s, c], dst_ref=e_recv.at[s, c],
                    send_sem=me_send.at[s, c], recv_sem=me_recv.at[s, c],
                    device_id=(g, mid), device_id_type=MESH,
                ).wait_recv()
                result[s, :, chunk(c)] = result[s, :, chunk(c)] - e_recv[s, c]
                write(s, c).start()

        for s in range(OWN):
            for j in range(last):
                feed_k(s, j).wait_send()
            for c in range(CHUNKS):
                feed_x(s, c).wait_send()

    @pl.when(is_mid)
    def _():
        def arrive_k(s, j, target):
            pltpu.make_async_remote_copy(
                src_ref=k_end.at[s, j], dst_ref=k_end.at[s, j],
                send_sem=em_send.at[s, j], recv_sem=em_recv.at[s, j], device_id=(g, end), device_id_type=MESH,
            ).wait_recv()

            @pl.loop(0, depth // STRIP)
            def _(i):
                first = pl.multiple_of(i * STRIP, STRIP)
                split_into(
                    k_stack, s, 3 * depth, depth, first, block(target), k_end[s, j, pl.ds(first, STRIP), :], (0, 0, 1)
                )

        def arrive_x(s, c):
            pltpu.make_async_remote_copy(
                src_ref=x_end.at[s, :, chunk(c)], dst_ref=x_end.at[s, :, chunk(c)],
                send_sem=em_send.at[s, last + c], recv_sem=em_recv.at[s, last + c],
                device_id=(g, end), device_id_type=MESH,
            ).wait_recv()

            @pl.loop(0, depth // STRIP)
            def _(i):
                first = pl.multiple_of(i * STRIP, STRIP)
                split_into(
                    x_stack, s, 3 * depth, depth, first, chunk(c), x_end[s, pl.ds(first, STRIP), chunk(c)], (0, 1, 0)
                )

        def produce(s):
            arrive_k(s, 0, far_end_of_mid)

            @pl.loop(0, CHUNKS)
            def _(c):
                arrive_x(s, c)
                p_send[s, 0, c] = contract(k_stack[s, :, block(far_end_of_mid)], x_stack[s, :, chunk(c)])
                cross(s, 0, c).start()

            arrive_k(s, 1, across)

            @pl.loop(0, CHUNKS)
            def _(c):
                p_send[s, 1, c] = contract(k_stack[s, :, block(across)], x_stack[s, :, chunk(c)])
                cross(s, 1, c).start()

        def forward(s):
            @pl.loop(0, CHUNKS)
            def _(c):
                part = contract(k_stack[s, own_terms, block(end)], x_stack[s, own_terms, chunk(c)])
                cross(s, 0, c).wait_recv()
                e_send[s, c] = p_recv[s, 0, c] + part
                deliver(s, c).start()

        def own_share(s):
            arrive_k(s, 2, t)
            migrate(s, 2).wait_recv()

            @pl.loop(0, CHUNKS)
            def _(c):
                result[s, :, chunk(c)] = stiffness(s, c) - contract(k_stack[s, :, block(t)], x_stack[s, :, chunk(c)])

        def finish(s):
            @pl.loop(0, CHUNKS)
            def _(c):
                cross(s, 1, c).wait_recv()
                result[s, :, chunk(c)] = result[s, :, chunk(c)] - p_recv[s, 1, c]
                write(s, c).start()

        for s in range(OWN):
            settle(s)
            stack_own(s)
        produce(0)
        send_stiffness()
        forward(0)
        produce(1)
        own_share(0)
        own_share(1)
        finish(0)
        forward(1)
        finish(1)
        for s in range(OWN):
            for c in range(CHUNKS):
                cross(s, 0, c).wait_send()
                cross(s, 1, c).wait_send()
                deliver(s, c).wait_send()

    for s in range(OWN):
        for kind in range(3):
            migrate(s, kind).wait_send()
        for c in range(CHUNKS):
            write(s, c).wait()


def line_body(coupling, interior_solve, boundary_stiffness, migration):
    home, depth, columns = interior_solve.shape
    rows = boundary_stiffness.shape[1]
    width = columns // CHUNKS
    f32, bf16 = jnp.float32, jnp.bfloat16
    share = (OWN, depth, columns)
    pieces = (OWN, CHUNKS, rows, width)
    dma = pltpu.SemaphoreType.DMA
    return pl.pallas_call(
        line_kernel,
        out_shape=jax.ShapeDtypeStruct((OWN, rows, columns), f32),
        in_specs=[pl.BlockSpec(memory_space=pltpu.SMEM)] + [pl.BlockSpec(memory_space=pl.ANY)] * 3,
        out_specs=pl.BlockSpec(memory_space=pl.ANY),
        scratch_shapes=[
            pltpu.VMEM((home, depth, columns), f32),
            pltpu.VMEM((home, depth, columns), f32),
            pltpu.VMEM((home, rows, columns), f32),
            pltpu.VMEM(share, f32),
            pltpu.VMEM(share, f32),
            pltpu.VMEM((OWN, rows, columns), f32),
            pltpu.VMEM(share, f32),
            pltpu.VMEM(share, f32),
            pltpu.VMEM((OWN, rows, columns), f32),
            pltpu.VMEM(share, f32),
            pltpu.VMEM(share, f32),
            pltpu.VMEM((OWN, LINE - 1, depth, rows), f32),
            pltpu.VMEM(share, f32),
            pltpu.VMEM((OWN, 6 * depth, columns), bf16),
            pltpu.VMEM((OWN, 6 * depth, columns), bf16),
            pltpu.VMEM((OWN, 2, CHUNKS, rows, width), f32),
            pltpu.VMEM((OWN, 2, CHUNKS, rows, width), f32),
            pltpu.VMEM(pieces, f32),
            pltpu.VMEM(pieces, f32),
            pltpu.VMEM((OWN, rows, columns), f32),
            dma((3,)),
            dma((OWN, 3)),
            dma((OWN, 3)),
            dma((OWN, LINE - 1 + CHUNKS)),
            dma((OWN, LINE - 1 + CHUNKS)),
            dma((OWN, 2, CHUNKS)),
            dma((OWN, 2, CHUNKS)),
            dma((OWN, CHUNKS)),
            dma((OWN, CHUNKS)),
            dma((OWN, CHUNKS)),
        ],
        compiler_params=pltpu.CompilerParams(
            collective_id=0, has_side_effects=True, vmem_limit_bytes=60 * 1024 * 1024
        ),
    )(migration, jnp.swapaxes(coupling, 1, 2), interior_solve, boundary_stiffness)


def solution(mesh):
    return jax.shard_map(
        line_body if mesh.shape["tile"] == LINE else portable_body,
        mesh=mesh,
        in_specs=(
            P("group", None, "tile"),
            P("group", "tile", None),
            P("group", "tile", None),
            P(),
        ),
        out_specs=P("group", "tile", None),
        check_vma=False,
    )
```

```python
import jax
import jax.numpy as jnp
from jax import lax
from jax.experimental import pallas as pl
from jax.experimental.pallas import tpu as pltpu
from jax.sharding import PartitionSpec as P

OWN = 2


def swapped(array, axis, distance):
    return lax.ppermute(array, axis, [(i, i ^ 1 << distance) for i in range(lax.axis_size(axis))])


def condense(coupling_cols, solve_rows, stiff_rows):
    product = lax.psum_scatter(
        jnp.dot(
            coupling_cols,
            solve_rows,
            precision=lax.Precision.HIGHEST,
            preferred_element_type=jnp.float32,
        ),
        "tile",
        scatter_dimension=0,
        tiled=True,
    )
    return stiff_rows - product


def select_slots(stacked, positions, present):
    chosen = jnp.take(stacked, positions, axis=0)
    shaped = present.reshape((-1,) + (1,) * (stacked.ndim - 1))
    return jnp.where(shaped, chosen, jnp.zeros_like(chosen))


def portable_body(coupling, interior_solve, boundary_stiffness, migration):
    home_count = coupling.shape[0]
    mygroup = lax.axis_index("group")
    partner = jnp.bitwise_xor(mygroup, 1)
    own_plan = lax.dynamic_slice_in_dim(migration, mygroup * home_count, home_count)
    slot_ids = jnp.arange(OWN, dtype=jnp.int32)
    local_ids = jnp.arange(home_count, dtype=jnp.int32)

    def locate(wanted):
        matches = own_plan[None, :] == wanted[:, None]
        positions = jnp.sum(jnp.where(matches, local_ids[None, :], 0), axis=1)
        return (positions, jnp.any(matches, axis=1))

    mine_index, mine_here = locate(mygroup * OWN + slot_ids)
    their_index, their_here = locate(partner * OWN + slot_ids)
    keep_mask = mine_here[:, None, None]
    outgoing = (
        select_slots(coupling, their_index, their_here),
        select_slots(interior_solve, their_index, their_here),
        select_slots(boundary_stiffness, their_index, their_here),
    )
    arrived = swapped((outgoing[0], outgoing[1], outgoing[2]), "group", 0)
    kept_coupling = jnp.where(keep_mask, jnp.take(coupling, mine_index, axis=0), arrived[0])
    kept_solve = jnp.where(keep_mask, jnp.take(interior_solve, mine_index, axis=0), arrived[1])
    kept_stiff = jnp.where(keep_mask, jnp.take(boundary_stiffness, mine_index, axis=0), arrived[2])
    result = jnp.stack(
        [condense(kept_coupling[slot], kept_solve[slot], kept_stiff[slot]) for slot in range(OWN)]
    )
    return result


MESH = pl.DeviceIdType.MESH
LINE = 4
CHUNKS = 8
STRIP = 16


def split_into(stack, slot, base, depth, rows, cols, value, order):
    high = value.astype(jnp.bfloat16)
    low = (value - high.astype(jnp.float32)).astype(jnp.bfloat16)
    for place, term in enumerate(order):
        at = pl.ds(base + place * depth + rows, value.shape[0])
        stack[slot, at, cols] = high if term == 0 else low


def contract(left, right):
    return lax.dot_general(left, right, (((0,), (0,)), ((), ())), preferred_element_type=jnp.float32)


def line_kernel(
    plan, k_hbm, x_hbm, b_hbm, result,
    k_home, x_home, b_home, k_out, x_out, b_out, k_in, x_in, b_in, k_got, x_got,
    k_end, x_end, k_stack, x_stack, p_send, p_recv, e_send, e_recv,
    load_sem, mig_send, mig_recv, em_send, em_recv, mm_send, mm_recv, me_send, me_recv,
):
    home, depth, columns = x_home.shape
    rows = b_home.shape[1]
    width = columns // CHUNKS
    last = LINE - 1
    g, t = lax.axis_index("group"), lax.axis_index("tile")
    partner = g + 1 - 2 * (g % 2)
    middle = (t % last + last - 1) // last
    is_end = middle == 0
    is_mid = middle == 1
    mid = 1 + t // last
    end = (t - 1) * last
    across = last - t
    far_end_of_end = last - t
    far_mid_of_end = last - mid
    far_end_of_mid = (2 - t) * last

    def block(index):
        return pl.ds(pl.multiple_of(index * rows, rows), rows)

    def chunk(index):
        return pl.ds(pl.multiple_of(index * width, width), width)

    loads = [
        pltpu.make_async_copy(src, dst, load_sem.at[i])
        for i, (src, dst) in enumerate(((k_hbm, k_home), (x_hbm, x_home), (b_hbm, b_home)))
    ]
    loads[0].start()
    loads[1].start()

    barrier = pltpu.get_barrier_semaphore()
    pl.semaphore_signal(barrier, inc=1, device_id=(partner, t), device_id_type=MESH)

    @pl.when(is_end)
    def _():
        pl.semaphore_signal(barrier, inc=1, device_id=(g, mid), device_id_type=MESH)

    @pl.when(is_mid)
    def _():
        pl.semaphore_signal(barrier, inc=1, device_id=(g, end), device_id_type=MESH)
        pl.semaphore_signal(barrier, inc=1, device_id=(g, across), device_id_type=MESH)

    def find(wanted):
        index, here = jnp.int32(0), jnp.int32(0)
        for j in range(home):
            hit = plan[g * home + j] == wanted
            index, here = jnp.where(hit, j, index), jnp.where(hit, 1, here)
        return index, here > 0

    mine = [find(g * OWN + s) for s in range(OWN)]
    theirs = [find(partner * OWN + s) for s in range(OWN)]

    def migrate(s, kind):
        src, dst = ((k_out, k_in), (x_out, x_in), (b_out, b_in))[kind]
        return pltpu.make_async_remote_copy(
            src_ref=src.at[s], dst_ref=dst.at[s], send_sem=mig_send.at[s, kind], recv_sem=mig_recv.at[s, kind],
            device_id=(partner, t), device_id_type=MESH,
        )

    def gather(src, dst, count):
        for s in range(OWN):
            @pl.loop(0, count // STRIP)
            def _(i):
                at = pl.ds(pl.multiple_of(i * STRIP, STRIP), STRIP)
                dst[s, at, :] = src[theirs[s][0], at, :]

    loads[0].wait()
    gather(k_home, k_out, depth)
    loads[1].wait()
    gather(x_home, x_out, depth)

    @pl.when(is_end)
    def _():
        pl.semaphore_wait(barrier, 2)

    @pl.when(is_mid)
    def _():
        pl.semaphore_wait(barrier, 3)

    for s in range(OWN):
        for kind in range(2):
            migrate(s, kind).start()
    loads[2].start()

    def settle(s, kind):
        migrate(s, kind).wait_recv()
        index, here = mine[s]
        got, own, arrived = ((k_got, k_home, k_in), (x_got, x_home, x_in))[kind]

        @pl.loop(0, depth // STRIP)
        def _(i):
            at = pl.ds(pl.multiple_of(i * STRIP, STRIP), STRIP)
            got[s, at, :] = jnp.where(here, own[index, at, :], arrived[s, at, :])

    def stack_own(s):
        @pl.loop(0, depth // STRIP)
        def _(i):
            first = pl.multiple_of(i * STRIP, STRIP)
            at = pl.ds(first, STRIP)
            everything = slice(None)
            split_into(k_stack, s, 0, depth, first, everything, k_got[s, at, :], (0, 0, 1))
            split_into(x_stack, s, 0, depth, first, everything, x_got[s, at, :], (0, 1, 0))

    def send_stiffness():
        loads[2].wait()
        gather(b_home, b_out, rows)
        for s in range(OWN):
            migrate(s, 2).start()

    def stiffness(s, c):
        index, here = mine[s]
        return jnp.where(here, b_home[index, :, chunk(c)], b_in[s, :, chunk(c)])

    def feed_k(s, j):
        target = (far_end_of_end, far_mid_of_end, mid)[j]
        return pltpu.make_async_remote_copy(
            src_ref=k_got.at[s, :, block(target)], dst_ref=k_end.at[s, j],
            send_sem=em_send.at[s, j], recv_sem=em_recv.at[s, j], device_id=(g, mid), device_id_type=MESH,
        )

    def feed_x(s, c):
        return pltpu.make_async_remote_copy(
            src_ref=x_got.at[s, :, chunk(c)], dst_ref=x_end.at[s, :, chunk(c)],
            send_sem=em_send.at[s, last + c], recv_sem=em_recv.at[s, last + c],
            device_id=(g, mid), device_id_type=MESH,
        )

    def cross(s, j, c):
        return pltpu.make_async_remote_copy(
            src_ref=p_send.at[s, j, c], dst_ref=p_recv.at[s, j, c],
            send_sem=mm_send.at[s, j, c], recv_sem=mm_recv.at[s, j, c],
            device_id=(g, across), device_id_type=MESH,
        )

    def deliver(s, c):
        return pltpu.make_async_remote_copy(
            src_ref=e_send.at[s, c], dst_ref=e_recv.at[s, c],
            send_sem=me_send.at[s, c], recv_sem=me_recv.at[s, c],
            device_id=(g, end), device_id_type=MESH,
        )

    own_terms = pl.ds(0, 3 * depth)

    @pl.when(is_end)
    def _():
        for s in range(OWN):
            settle(s, 0)
            feed_k(s, 0).start()
            settle(s, 1)
            for c in range(CHUNKS):
                feed_x(s, c).start()
            feed_k(s, 1).start()
            feed_k(s, 2).start()
        send_stiffness()
        for s in range(OWN):
            stack_own(s)
        for s in range(OWN):
            migrate(s, 2).wait_recv()

            @pl.loop(0, CHUNKS)
            def _(c):
                result[s, :, chunk(c)] = stiffness(s, c) - contract(
                    k_stack[s, own_terms, block(t)], x_stack[s, own_terms, chunk(c)]
                )

        for s in range(OWN):
            @pl.loop(0, CHUNKS)
            def _(c):
                pltpu.make_async_remote_copy(
                    src_ref=e_send.at[s, c], dst_ref=e_recv.at[s, c],
                    send_sem=me_send.at[s, c], recv_sem=me_recv.at[s, c],
                    device_id=(g, mid), device_id_type=MESH,
                ).wait_recv()
                result[s, :, chunk(c)] = result[s, :, chunk(c)] - e_recv[s, c]

        for s in range(OWN):
            for j in range(last):
                feed_k(s, j).wait_send()
            for c in range(CHUNKS):
                feed_x(s, c).wait_send()

    @pl.when(is_mid)
    def _():
        def arrive_k(s, j, target):
            pltpu.make_async_remote_copy(
                src_ref=k_end.at[s, j], dst_ref=k_end.at[s, j],
                send_sem=em_send.at[s, j], recv_sem=em_recv.at[s, j], device_id=(g, end), device_id_type=MESH,
            ).wait_recv()

            @pl.loop(0, depth // STRIP)
            def _(i):
                first = pl.multiple_of(i * STRIP, STRIP)
                split_into(
                    k_stack, s, 3 * depth, depth, first, block(target), k_end[s, j, pl.ds(first, STRIP), :], (0, 0, 1)
                )

        def arrive_x(s, c):
            pltpu.make_async_remote_copy(
                src_ref=x_end.at[s, :, chunk(c)], dst_ref=x_end.at[s, :, chunk(c)],
                send_sem=em_send.at[s, last + c], recv_sem=em_recv.at[s, last + c],
                device_id=(g, end), device_id_type=MESH,
            ).wait_recv()

            @pl.loop(0, depth // STRIP)
            def _(i):
                first = pl.multiple_of(i * STRIP, STRIP)
                split_into(
                    x_stack, s, 3 * depth, depth, first, chunk(c), x_end[s, pl.ds(first, STRIP), chunk(c)], (0, 1, 0)
                )

        def produce(s):
            arrive_k(s, 0, far_end_of_mid)

            @pl.loop(0, CHUNKS)
            def _(c):
                arrive_x(s, c)
                p_send[s, 0, c] = contract(k_stack[s, :, block(far_end_of_mid)], x_stack[s, :, chunk(c)])
                cross(s, 0, c).start()

            arrive_k(s, 1, across)

            @pl.loop(0, CHUNKS)
            def _(c):
                p_send[s, 1, c] = contract(k_stack[s, :, block(across)], x_stack[s, :, chunk(c)])
                cross(s, 1, c).start()

        def forward(s):
            @pl.loop(0, CHUNKS)
            def _(c):
                part = contract(k_stack[s, own_terms, block(end)], x_stack[s, own_terms, chunk(c)])
                cross(s, 0, c).wait_recv()
                e_send[s, c] = p_recv[s, 0, c] + part
                deliver(s, c).start()

        def own_share(s):
            arrive_k(s, 2, t)
            migrate(s, 2).wait_recv()

            @pl.loop(0, CHUNKS)
            def _(c):
                result[s, :, chunk(c)] = stiffness(s, c) - contract(k_stack[s, :, block(t)], x_stack[s, :, chunk(c)])

        def finish(s):
            @pl.loop(0, CHUNKS)
            def _(c):
                cross(s, 1, c).wait_recv()
                result[s, :, chunk(c)] = result[s, :, chunk(c)] - p_recv[s, 1, c]

        for s in range(OWN):
            settle(s, 0)
            settle(s, 1)
            stack_own(s)
        produce(0)
        send_stiffness()
        forward(0)
        produce(1)
        own_share(0)
        own_share(1)
        finish(0)
        forward(1)
        finish(1)
        for s in range(OWN):
            for c in range(CHUNKS):
                cross(s, 0, c).wait_send()
                cross(s, 1, c).wait_send()
                deliver(s, c).wait_send()

    for s in range(OWN):
        for kind in range(3):
            migrate(s, kind).wait_send()


def line_body(coupling, interior_solve, boundary_stiffness, migration):
    home, depth, columns = interior_solve.shape
    rows = boundary_stiffness.shape[1]
    width = columns // CHUNKS
    f32, bf16 = jnp.float32, jnp.bfloat16
    share = (OWN, depth, columns)
    pieces = (OWN, CHUNKS, rows, width)
    dma = pltpu.SemaphoreType.DMA
    return pl.pallas_call(
        line_kernel,
        out_shape=pltpu.VMEM((OWN, rows, columns), f32),
        in_specs=[pl.BlockSpec(memory_space=pltpu.SMEM)] + [pl.BlockSpec(memory_space=pl.ANY)] * 3,
        out_specs=pl.BlockSpec(memory_space=pltpu.VMEM),
        scratch_shapes=[
            pltpu.VMEM((home, depth, columns), f32),
            pltpu.VMEM((home, depth, columns), f32),
            pltpu.VMEM((home, rows, columns), f32),
            pltpu.VMEM(share, f32),
            pltpu.VMEM(share, f32),
            pltpu.VMEM((OWN, rows, columns), f32),
            pltpu.VMEM(share, f32),
            pltpu.VMEM(share, f32),
            pltpu.VMEM((OWN, rows, columns), f32),
            pltpu.VMEM(share, f32),
            pltpu.VMEM(share, f32),
            pltpu.VMEM((OWN, LINE - 1, depth, rows), f32),
            pltpu.VMEM(share, f32),
            pltpu.VMEM((OWN, 6 * depth, columns), bf16),
            pltpu.VMEM((OWN, 6 * depth, columns), bf16),
            pltpu.VMEM((OWN, 2, CHUNKS, rows, width), f32),
            pltpu.VMEM((OWN, 2, CHUNKS, rows, width), f32),
            pltpu.VMEM(pieces, f32),
            pltpu.VMEM(pieces, f32),
            dma((3,)),
            dma((OWN, 3)),
            dma((OWN, 3)),
            dma((OWN, LINE - 1 + CHUNKS)),
            dma((OWN, LINE - 1 + CHUNKS)),
            dma((OWN, 2, CHUNKS)),
            dma((OWN, 2, CHUNKS)),
            dma((OWN, CHUNKS)),
            dma((OWN, CHUNKS)),
        ],
        compiler_params=pltpu.CompilerParams(
            collective_id=0, has_side_effects=True, vmem_limit_bytes=60 * 1024 * 1024
        ),
    )(migration, jnp.swapaxes(coupling, 1, 2), interior_solve, boundary_stiffness)


def solution(mesh):
    return jax.shard_map(
        line_body if mesh.shape["tile"] == LINE else portable_body,
        mesh=mesh,
        in_specs=(
            P("group", None, "tile"),
            P("group", "tile", None),
            P("group", "tile", None),
            P(),
        ),
        out_specs=P("group", "tile", None),
        check_vma=False,
    )
```
